32 devices in a mesh: dp: 1 (over z), col: 4 (over y), row: 8 (over x, core).
Axes of the slice: x: 4, y: 4, z: 1, core: 2. Of those that a mesh axis runs over, the one named last changes fastest.
The devices are a block of a 4x4x8 slice.
Arguments:
- x_tok: bfloat16 [16384, 5120], P(('dp', 'row'), 'col')
- ln_gamma: float32 [5120], P('col')
- w_in: bfloat16 [5120, 13824], P('row', 'col')
- w_out: bfloat16 [13824, 5120], P('row', 'col')
Outputs:
- output: bfloat16 [16384, 5120], P(('dp', 'row'), 'col')
All inputs are finite; a program needn't handle non-finite values.
Results may differ from the reference program's by a relative error of at most 0.00113.
Values are sent between devices in bfloat16 or wider.
A program may use at most 768 MiB of HBM per device.

```python
import jax
import jax.numpy as jnp
from jax import lax

TOKENS = 16384
D_MODEL = 5120
D_HIDDEN = 13824
BLOCK_ROWS = 256
LN_EPS = 1e-5


def setup_inputs(seed: int = 0, part: int = 0) -> dict:
    part_key = jax.random.fold_in(jax.random.key(seed), part)
    key_noise, key_mean, key_slope, key_scale = jax.random.split(part_key, 4)
    key_gamma, key_in, key_out = jax.random.split(jax.random.key(seed + 1), 3)
    feat_ramp = jnp.linspace(-1.0, 1.0, D_MODEL, dtype=jnp.float32)
    row_mean = 0.5 + jax.random.normal(key_mean, (TOKENS, 1), jnp.float32)
    row_slope = jax.random.normal(key_slope, (TOKENS, 1), jnp.float32)
    col_scale = (0.4 + 0.6 * (feat_ramp + 1.0)) * (0.75 + 0.5 * jax.random.uniform(key_scale, (D_MODEL,), jnp.float32))
    base_noise = jax.random.normal(key_noise, (TOKENS, D_MODEL), jnp.float32)
    x_tok = (row_mean + row_slope * feat_ramp + col_scale * base_noise).astype(jnp.bfloat16)
    ln_gamma = 1.0 + 0.5 * jax.random.normal(key_gamma, (D_MODEL,), jnp.float32)
    w_in = (jax.random.normal(key_in, (D_MODEL, D_HIDDEN), jnp.float32) * D_MODEL ** -0.5).astype(jnp.bfloat16)
    w_out = (jax.random.normal(key_out, (D_HIDDEN, D_MODEL), jnp.float32) * (2.0 * D_HIDDEN ** -0.5)).astype(jnp.bfloat16)
    return {"x_tok": x_tok, "ln_gamma": ln_gamma, "w_in": w_in, "w_out": w_out}


def mlp_rows(x_rows, ln_gamma, w_in, w_out):
    x_f32 = x_rows.astype(jnp.float32)
    mean_row = jnp.mean(x_f32, axis=1, keepdims=True)
    var_row = jnp.mean(x_f32 * x_f32, axis=1, keepdims=True) - mean_row * mean_row
    normed = ((x_f32 - mean_row) * lax.rsqrt(var_row + LN_EPS) * ln_gamma).astype(jnp.bfloat16)
    pre_act = jnp.dot(normed, w_in, preferred_element_type=jnp.float32)
    hidden = jax.nn.gelu(pre_act, approximate=True).astype(jnp.bfloat16)
    branch = jnp.dot(hidden, w_out, preferred_element_type=jnp.float32)
    return (x_f32 + branch).astype(jnp.bfloat16)


def reference(x_tok, ln_gamma, w_in, w_out):
    row_blocks = x_tok.reshape(TOKENS // BLOCK_ROWS, BLOCK_ROWS, D_MODEL)
    out_blocks = lax.map(lambda row_block: mlp_rows(row_block, ln_gamma, w_in, w_out), row_blocks)
    return out_blocks.reshape(TOKENS, D_MODEL)
```

```python
import jax
import jax.numpy as jnp
from jax import lax
from jax.sharding import PartitionSpec as P

LN_EPS = 1e-5
CHUNKS = 2


def solution(mesh):
    n_col = mesh.shape["col"]
    tok_spec = P(("dp", "row"), "col")
    near_pairs = [(i, i ^ 1) for i in range(n_col)]
    far_pairs = [(i, n_col - 1 - i) for i in range(n_col)]

    def near(v):
        return lax.ppermute(v, "col", near_pairs)

    def far(v):
        return lax.ppermute(v, "col", far_pairs)

    def local_block(x_loc, gamma_loc, w_in_loc, w_out_loc):
        rows, width = x_loc.shape
        d_model = width * n_col
        hid_loc = w_in_loc.shape[1]
        d_hidden = hid_loc * n_col
        half = rows // 2
        step = half // CHUNKS
        me = lax.axis_index("col")
        side = me // 2
        owners = [me, me ^ 1, n_col - 1 - me, me ^ 2]

        w_in_panel = lax.all_gather(w_in_loc, "row", axis=0, tiled=True)

        x_mine = lax.dynamic_slice(x_loc, (side * half, 0), (half, width))
        x_other = lax.dynamic_slice(x_loc, ((1 - side) * half, 0), (half, width))
        g_near, g_far = near(gamma_loc), far(gamma_loc)
        g_opp = near(g_far)
        gammas = [gamma_loc, g_near, g_far, g_opp]
        a1 = near(x_mine)
        b1 = far(x_other)
        a2 = near(b1)
        b2 = far(x_mine)
        a3 = near(x_other)
        b3 = far(a1)
        a2, b2, w_out_tied = lax.optimization_barrier((a2, b2, w_out_loc))
        w_out_far = far(w_out_tied)

        w_far_panel = lax.all_gather(w_out_far, "row", axis=0, tiled=True)
        w_own_panel = lax.all_gather(w_out_loc, "row", axis=0, tiled=True)

        def normed(blocks):
            sums = sum(jnp.sum(b.astype(jnp.float32), axis=1, keepdims=True) for b in blocks)
            squares = sum(jnp.sum(jnp.square(b.astype(jnp.float32)), axis=1, keepdims=True) for b in blocks)
            mean = sums / d_model
            scale = lax.rsqrt(squares / d_model - mean * mean + LN_EPS)
            z = jnp.zeros((blocks[0].shape[0], d_model), jnp.bfloat16)
            for b, g, owner in zip(blocks, gammas, owners):
                piece = ((b.astype(jnp.float32) - mean) * scale * g).astype(jnp.bfloat16)
                z = lax.dynamic_update_slice(z, piece, (0, owner * width))
            return z

        def hidden(blocks, c):
            z = normed([b[c * step:(c + 1) * step] for b in blocks])
            pre = jnp.dot(z, w_in_panel, preferred_element_type=jnp.float32)
            return jax.nn.gelu(pre, approximate=True).astype(jnp.bfloat16)

        h_mine = [hidden([x_mine, a1, b1, a2], c) for c in range(CHUNKS)]
        h_near = [near(h) for h in h_mine]
        h_other = [hidden([x_other, a3, b2, b3], c) for c in range(CHUNKS)]
        h_far = [far(h) for h in h_other]
        h_opp = [near(h) for h in h_far]

        own_parts, far_parts = [], []
        for c in range(CHUNKS):
            panel = jnp.zeros((step, d_hidden), jnp.bfloat16)
            for piece, owner in zip((h_mine[c], h_near[c], h_far[c], h_opp[c]), owners):
                panel = lax.dynamic_update_slice(panel, piece, (0, owner * hid_loc))
            span = slice(c * step, (c + 1) * step)
            branch = jnp.dot(panel, w_far_panel, preferred_element_type=jnp.float32)
            far_parts.append(far((b1[span].astype(jnp.float32) + branch).astype(jnp.bfloat16)))
            branch = jnp.dot(panel, w_own_panel, preferred_element_type=jnp.float32)
            own_parts.append((x_mine[span].astype(jnp.float32) + branch).astype(jnp.bfloat16))

        y = jnp.zeros((rows, width), jnp.bfloat16)
        for c in range(CHUNKS):
            y = lax.dynamic_update_slice(y, own_parts[c], (side * half + c * step, 0))
            y = lax.dynamic_update_slice(y, far_parts[c], ((1 - side) * half + c * step, 0))
        return y

    return jax.shard_map(local_block, mesh=mesh, in_specs=(tok_spec, P("col"), P("row", "col"), P("row", "col")), out_specs=tok_spec, check_vma=False)
```

```python
import jax
import jax.numpy as jnp
from jax import lax
from jax.experimental import pallas as pl
from jax.experimental.pallas import tpu as pltpu
from jax.sharding import PartitionSpec as P

LN_EPS = 1e-5
CHUNKS = 4
FIRST_COLS = 768
VMEM_LIMIT = 56 * 1024 * 1024


def up_kernel(meta, *refs):
    blocks, gammas = refs[0:4], refs[4:8]
    w_ref, h_ref, z_ref = refs[8:]
    width = blocks[0].shape[1]
    d_model = z_ref.shape[1]

    @pl.when(pl.program_id(0) == 0)
    def _():
        sums, squares = 0.0, 0.0
        for b in blocks:
            v = b[...].astype(jnp.float32)
            sums += jnp.sum(v, axis=1, keepdims=True)
            squares += jnp.sum(v * v, axis=1, keepdims=True)
        mean = sums / d_model
        scale = lax.rsqrt(squares / d_model - mean * mean + LN_EPS)
        for j, (b, g) in enumerate(zip(blocks, gammas)):
            piece = (b[...].astype(jnp.float32) - mean) * scale * g[...]
            z_ref[:, pl.ds(pl.multiple_of(meta[j] * width, 128), width)] = piece.astype(jnp.bfloat16)

    pre = jnp.dot(z_ref[...], w_ref[...], preferred_element_type=jnp.float32)
    h_ref[...] = jax.nn.gelu(pre, approximate=True).astype(jnp.bfloat16)


def up(meta, c, step, blocks, gammas, w, tile):
    d_model, hid = w.shape
    width = blocks[0].shape[1]
    return pl.pallas_call(
        up_kernel,
        grid_spec=pltpu.PrefetchScalarGridSpec(
            num_scalar_prefetch=1,
            grid=(hid // tile,),
            in_specs=[pl.BlockSpec((step, width), lambda n, m: (c, 0))] * 4
            + [pl.BlockSpec((1, width), lambda n, m: (0, 0))] * 4
            + [pl.BlockSpec((d_model, tile), lambda n, m: (0, n))],
            out_specs=pl.BlockSpec((step, tile), lambda n, m: (0, n)),
            scratch_shapes=[pltpu.VMEM((step, d_model), jnp.bfloat16)],
        ),
        out_shape=jax.ShapeDtypeStruct((step, hid), jnp.bfloat16),
        compiler_params=pltpu.CompilerParams(vmem_limit_bytes=VMEM_LIMIT),
        cost_estimate=pl.CostEstimate(flops=2 * step * d_model * hid, bytes_accessed=2 * d_model * hid, transcendentals=step * hid),
    )(meta, *blocks, *gammas, w)


def down_kernel(meta, *refs):
    hs, ws, x_ref, y_ref = refs[0:4], refs[4:8], refs[8], refs[9]
    total = x_ref[...].astype(jnp.float32)
    branch = jnp.dot(hs[0][...], ws[0][...], preferred_element_type=jnp.float32)
    for h, w in zip(hs[1:], ws[1:]):
        branch += jnp.dot(h[...], w[...], preferred_element_type=jnp.float32)
    y_ref[...] = (total + branch).astype(jnp.bfloat16)


def down(meta, c, step, hs, w, x, x_col, tile):
    hid = hs[0].shape[1]
    cols = w.shape[1]

    def w_spec(j):
        return pl.BlockSpec((hid, tile), lambda n, m: (m[j], n))

    return pl.pallas_call(
        down_kernel,
        grid_spec=pltpu.PrefetchScalarGridSpec(
            num_scalar_prefetch=1,
            grid=(cols // tile,),
            in_specs=[pl.BlockSpec((step, hid), lambda n, m: (0, 0))] * 4
            + [w_spec(j) for j in range(4)]
            + [pl.BlockSpec((step, tile), lambda n, m: (c, x_col // tile + n))],
            out_specs=pl.BlockSpec((step, tile), lambda n, m: (0, n)),
        ),
        out_shape=jax.ShapeDtypeStruct((step, cols), jnp.bfloat16),
        compiler_params=pltpu.CompilerParams(vmem_limit_bytes=VMEM_LIMIT),
        cost_estimate=pl.CostEstimate(flops=8 * step * hid * cols, bytes_accessed=8 * hid * cols, transcendentals=0),
    )(meta, *hs, *[w] * 4, x)


def solution(mesh):
    n_col = mesh.shape["col"]
    tok_spec = P(("dp", "row"), "col")
    near_pairs = [(i, i ^ 1) for i in range(n_col)]
    far_pairs = [(i, n_col - 1 - i) for i in range(n_col)]

    def near(v):
        return lax.ppermute(v, "col", near_pairs)

    def far(v):
        return lax.ppermute(v, "col", far_pairs)

    def gather(v):
        return lax.all_gather(v, "row", axis=0, tiled=True)

    def local_block(x_loc, gamma_loc, w_in_loc, w_out_loc):
        rows, width = x_loc.shape
        half = rows // 2
        step = half // CHUNKS
        me = lax.axis_index("col")
        side = me // 2
        meta = jnp.stack([me, me ^ 1, n_col - 1 - me, me ^ 2]).astype(jnp.int32)

        w_in_panel = gather(w_in_loc)
        own_first = gather(w_out_loc[:, :FIRST_COLS])

        x_mine = lax.dynamic_slice(x_loc, (side * half, 0), (half, width))
        x_other = lax.dynamic_slice(x_loc, ((1 - side) * half, 0), (half, width))
        gamma_row = gamma_loc.reshape(1, width)
        g_near, g_far = near(gamma_row), far(gamma_row)
        g_opp = near(g_far)
        gammas = [gamma_row, g_near, g_far, g_opp]
        a1 = near(x_mine)
        b1 = far(x_other)
        a3 = near(x_other)
        b2 = far(x_mine)
        a1, b1, a3, b2, *gammas = lax.optimization_barrier((a1, b1, a3, b2, *gammas))
        a2 = near(b1)
        b3 = far(a1)
        a2, b3, w_out_tied = lax.optimization_barrier((a2, b3, w_out_loc))
        w_out_far = far(w_out_tied)

        tile_up = 384
        h_mine, h_near, h_other, h_far = [], [], [], []
        for c in range(CHUNKS):
            h_mine.append(up(meta, c, step, [x_mine, a1, b1, a2], gammas, w_in_panel, tile_up))
            h_near.append(near(h_mine[c]))
        for c in range(CHUNKS):
            h_other.append(up(meta, c, step, [x_other, a3, b2, b3], gammas, w_in_panel, tile_up))
            if c == CHUNKS - 1:
                w_out_far, h_other[c] = lax.optimization_barrier((w_out_far, h_other[c]))
            h_far.append(far(h_other[c]))
        far_panel = gather(w_out_far)
        w_last, h_far[0] = lax.optimization_barrier((w_out_loc[:, FIRST_COLS:], h_far[0]))
        own_last = gather(w_last)
        h_opp = [near(h) for h in h_far]

        y = jnp.zeros((rows, width), jnp.bfloat16)
        for c in range(CHUNKS):
            hs = [h_mine[c], h_near[c], h_far[c], h_opp[c]]
            sent = down(meta, c, step, hs, far_panel, b1, 0, 256)
            sent = far(sent)
            first = down(meta, c, step, hs, own_first, x_mine, 0, 256)
            last = down(meta, c, step, hs, own_last, x_mine, FIRST_COLS, 256)
            y = lax.dynamic_update_slice(y, first, (side * half + c * step, 0))
            y = lax.dynamic_update_slice(y, last, (side * half + c * step, FIRST_COLS))
            y = lax.dynamic_update_slice(y, sent, ((1 - side) * half + c * step, 0))
        return y

    return jax.shard_map(local_block, mesh=mesh, in_specs=(tok_spec, P("col"), P("row", "col"), P("row", "col")), out_specs=tok_spec, check_vma=False)
```

```python
import jax
import jax.numpy as jnp
from jax import lax
from jax.experimental import pallas as pl
from jax.experimental.pallas import tpu as pltpu
from jax.sharding import PartitionSpec as P


LN_EPS = 1e-5
CHUNKS = 4
FIRST_COLS = 768
VMEM_LIMIT = 58 * 1024 * 1024
UP_SPLIT, UP_TILE = 4, 512
DOWN_SPLIT, DOWN_TILE = 2, 256


def up_kernel(meta, *refs):
    blocks, gammas, ws = refs[0:4], refs[4:8], refs[8:8 + UP_SPLIT]
    h_refs, z_ref = refs[8 + UP_SPLIT:-1], refs[-1]
    width = blocks[0].shape[1]
    d_model = z_ref.shape[1]

    @pl.when(pl.program_id(0) == 0)
    def _():
        sums, squares = 0.0, 0.0
        for b in blocks:
            v = b[...].astype(jnp.float32)
            sums += jnp.sum(v, axis=1, keepdims=True)
            squares += jnp.sum(v * v, axis=1, keepdims=True)
        mean = sums / d_model
        scale = lax.rsqrt(squares / d_model - mean * mean + LN_EPS)
        for j, (b, g) in enumerate(zip(blocks, gammas)):
            piece = (b[...].astype(jnp.float32) - mean) * scale * g[...]
            z_ref[:, pl.ds(pl.multiple_of(meta[j] * width, 128), width)] = piece.astype(jnp.bfloat16)

    depth = d_model // UP_SPLIT
    pre = jnp.dot(z_ref[:, :depth], ws[0][...], preferred_element_type=jnp.float32)
    for s in range(1, UP_SPLIT):
        pre += jnp.dot(z_ref[:, s * depth:(s + 1) * depth], ws[s][...], preferred_element_type=jnp.float32)
    h = jax.nn.gelu(pre, approximate=True).astype(jnp.bfloat16)
    piece = h_refs[0].shape[0]
    for i, h_ref in enumerate(h_refs):
        h_ref[...] = h[i * piece:(i + 1) * piece]


def up(meta, pair, step, blocks, gammas, w):
    d_model, hid = w.shape
    width = blocks[0].shape[1]
    return pl.pallas_call(
        up_kernel,
        grid_spec=pltpu.PrefetchScalarGridSpec(
            num_scalar_prefetch=1,
            grid=(pl.cdiv(hid, UP_TILE),),
            in_specs=[pl.BlockSpec((2 * step, width), lambda n, m: (pair, 0))] * 4
            + [pl.BlockSpec((1, width), lambda n, m: (0, 0))] * 4
            + [pl.BlockSpec((d_model // UP_SPLIT, UP_TILE), lambda n, m, s=s: (s, n)) for s in range(UP_SPLIT)],
            out_specs=[pl.BlockSpec((step, UP_TILE), lambda n, m: (0, n))] * 2,
            scratch_shapes=[pltpu.VMEM((2 * step, d_model), jnp.bfloat16)],
        ),
        out_shape=[jax.ShapeDtypeStruct((step, hid), jnp.bfloat16)] * 2,
        compiler_params=pltpu.CompilerParams(vmem_limit_bytes=VMEM_LIMIT),
        cost_estimate=pl.CostEstimate(flops=4 * step * d_model * hid, bytes_accessed=2 * d_model * hid, transcendentals=2 * step * hid),
    )(meta, *blocks, *gammas, *[w] * UP_SPLIT)


def down_kernel(meta, *refs):
    n_w = 4 * DOWN_SPLIT
    x_ref, y_ref = refs[-2], refs[-1]
    ws, hs = refs[-2 - n_w:-2], refs[:-2 - n_w]
    pieces = len(hs) // 4
    depth = ws[0].shape[0]
    branch = None
    for j in range(4):
        for s in range(DOWN_SPLIT):
            parts = [h[:, s * depth:(s + 1) * depth] for h in hs[j * pieces:(j + 1) * pieces]]
            lhs = parts[0] if pieces == 1 else jnp.concatenate(parts, axis=0)
            term = jnp.dot(lhs, ws[j * DOWN_SPLIT + s][...], preferred_element_type=jnp.float32)
            branch = term if branch is None else branch + term
    y_ref[...] = (x_ref[...].astype(jnp.float32) + branch).astype(jnp.bfloat16)


def down(meta, at, step, hs, w, x, x_col):
    pieces = len(hs[0])
    hid = hs[0][0].shape[1]
    cols = w.shape[1]
    rows = step * pieces
    w_specs = [
        pl.BlockSpec((hid // DOWN_SPLIT, DOWN_TILE), lambda n, m, j=j, s=s: (m[j] * DOWN_SPLIT + s, n))
        for j in range(4) for s in range(DOWN_SPLIT)
    ]
    return pl.pallas_call(
        down_kernel,
        grid_spec=pltpu.PrefetchScalarGridSpec(
            num_scalar_prefetch=1,
            grid=(cols // DOWN_TILE,),
            in_specs=[pl.BlockSpec((step, hid), lambda n, m: (0, 0))] * (4 * pieces)
            + w_specs
            + [pl.BlockSpec((rows, DOWN_TILE), lambda n, m: (at, x_col // DOWN_TILE + n))],
            out_specs=pl.BlockSpec((rows, DOWN_TILE), lambda n, m: (0, n)),
        ),
        out_shape=jax.ShapeDtypeStruct((rows, cols), jnp.bfloat16),
        compiler_params=pltpu.CompilerParams(vmem_limit_bytes=VMEM_LIMIT),
        cost_estimate=pl.CostEstimate(flops=8 * rows * hid * cols, bytes_accessed=8 * hid * cols, transcendentals=0),
    )(meta, *[h for owner in hs for h in owner], *[w] * (4 * DOWN_SPLIT), x)


def copy_kernel(in_ref, out_ref):
    out_ref[...] = in_ref[...]


def solution(mesh):
    n_col = mesh.shape["col"]
    tok_spec = P(("dp", "row"), "col")
    near_pairs = [(i, i ^ 1) for i in range(n_col)]
    far_pairs = [(i, n_col - 1 - i) for i in range(n_col)]

    def near(v):
        return lax.ppermute(v, "col", near_pairs)

    def far(v):
        return lax.ppermute(v, "col", far_pairs)

    def gather(v):
        return lax.all_gather(v, "row", axis=0, tiled=True)

    def local_block(x_loc, gamma_loc, w_in_loc, w_out_loc):
        rows, width = x_loc.shape
        half = rows // 2
        step = half // CHUNKS
        me = lax.axis_index("col")
        side = me // 2
        meta = jnp.stack([me, me ^ 1, n_col - 1 - me, me ^ 2]).astype(jnp.int32)

        w_in_panel = gather(w_in_loc)

        x_mine = lax.dynamic_slice(x_loc, (side * half, 0), (half, width))
        x_other = lax.dynamic_slice(x_loc, ((1 - side) * half, 0), (half, width))
        a1 = near(x_mine)
        b1 = far(x_other)
        w_out_far = far(w_out_loc)
        b2 = far(x_mine)
        a2 = near(b1)
        a3 = near(x_other)
        b3 = far(a1)
        gamma_row = gamma_loc.reshape(1, width)
        g_near, g_far = near(gamma_row), far(gamma_row)
        g_opp = near(g_far)
        gammas = [gamma_row, g_near, g_far, g_opp]

        marked = pl.pallas_call(copy_kernel, out_shape=jax.ShapeDtypeStruct(gamma_row.shape, gamma_row.dtype))(gamma_row)
        w_out_far, marked = lax.optimization_barrier((w_out_far, marked))
        other_gammas = [marked] + gammas[1:]

        far_panel = gather(w_out_far)
        w_out_far, w_first = lax.optimization_barrier((w_out_far, w_out_loc[:, :FIRST_COLS]))
        own_first = gather(w_first)

        h_mine, h_near, h_other, h_far = [], [], [], []
        for p in range(CHUNKS // 2):
            h_mine += up(meta, p, step, [x_mine, a1, b1, a2], gammas, w_in_panel)
            h_near += [near(h_mine[c]) for c in (2 * p, 2 * p + 1)]
        for p in range(CHUNKS // 2):
            h_other += up(meta, p, step, [x_other, a3, b2, b3], other_gammas, w_in_panel)
            h_far += [far(h_other[c]) for c in (2 * p, 2 * p + 1)]
        h_opp = [near(h) for h in h_far]
        w_last, h_opp[1] = lax.optimization_barrier((w_out_loc[:, FIRST_COLS:], h_opp[1]))
        own_last = gather(w_last)

        def call(chunks, w, x, x_col):
            hs = [[h[c] for c in chunks] for h in (h_mine, h_near, h_far, h_opp)]
            return down(meta, chunks[0] // len(chunks), step, hs, w, x, x_col)

        y = jnp.zeros((rows, width), jnp.bfloat16)
        for chunks in ((0, 1), (2,), (3,)):
            part = far(call(chunks, far_panel, b1, 0))
            y = lax.dynamic_update_slice(y, part, ((1 - side) * half + chunks[0] * step, 0))
        for chunks in ((0, 1), (2, 3)):
            part = call(chunks, own_first, x_mine, 0)
            y = lax.dynamic_update_slice(y, part, (side * half + chunks[0] * step, 0))
            part = call(chunks, own_last, x_mine, FIRST_COLS)
            y = lax.dynamic_update_slice(y, part, (side * half + chunks[0] * step, FIRST_COLS))
        return y

    return jax.shard_map(local_block, mesh=mesh, in_specs=(tok_spec, P("col"), P("row", "col"), P("row", "col")), out_specs=tok_spec, check_vma=False)
```

```python
import jax
import jax.numpy as jnp
from jax import lax
from jax.experimental import pallas as pl
from jax.experimental.pallas import tpu as pltpu
from jax.sharding import PartitionSpec as P


LN_EPS = 1e-5
CHUNKS = 4
FIRST_COLS = 1024
NORM_ROWS = 128
VMEM_LIMIT = 58 * 1024 * 1024
UP_SPLIT, UP_TILE = 4, 512
DOWN_SPLIT, DOWN_TILE = 2, 256


def norm_kernel(meta, *refs):
    blocks, gammas, z_ref = refs[0:4], refs[4:8], refs[8]
    width = blocks[0].shape[1]
    d_model = z_ref.shape[1]
    sums, squares = 0.0, 0.0
    for b in blocks:
        v = b[...].astype(jnp.float32)
        sums += jnp.sum(v, axis=1, keepdims=True)
        squares += jnp.sum(v * v, axis=1, keepdims=True)
    mean = sums / d_model
    scale = lax.rsqrt(squares / d_model - mean * mean + LN_EPS)
    for j, (b, g) in enumerate(zip(blocks, gammas)):
        piece = (b[...].astype(jnp.float32) - mean) * scale * g[...]
        z_ref[:, pl.ds(pl.multiple_of(meta[j] * width, 128), width)] = piece.astype(jnp.bfloat16)


def norm(meta, blocks, gammas):
    rows, width = blocks[0].shape
    d_model = width * 4
    return pl.pallas_call(
        norm_kernel,
        grid_spec=pltpu.PrefetchScalarGridSpec(
            num_scalar_prefetch=1,
            grid=(rows // NORM_ROWS,),
            in_specs=[pl.BlockSpec((NORM_ROWS, width), lambda i, m: (i, 0))] * 4
            + [pl.BlockSpec((1, width), lambda i, m: (0, 0))] * 4,
            out_specs=pl.BlockSpec((NORM_ROWS, d_model), lambda i, m: (i, 0)),
        ),
        out_shape=jax.ShapeDtypeStruct((rows, d_model), jnp.bfloat16),
        compiler_params=pltpu.CompilerParams(vmem_limit_bytes=VMEM_LIMIT),
        cost_estimate=pl.CostEstimate(flops=64 * rows * d_model, bytes_accessed=4 * rows * d_model, transcendentals=rows),
    )(meta, *blocks, *gammas)


def up_kernel(z_ref, *refs):
    ws, h_refs = refs[:UP_SPLIT], refs[UP_SPLIT:]
    depth = ws[0].shape[0]
    pre = jnp.dot(z_ref[:, :depth], ws[0][...], preferred_element_type=jnp.float32)
    for s in range(1, UP_SPLIT):
        pre += jnp.dot(z_ref[:, s * depth:(s + 1) * depth], ws[s][...], preferred_element_type=jnp.float32)
    h = jax.nn.gelu(pre, approximate=True).astype(jnp.bfloat16)
    piece = h_refs[0].shape[0]
    for i, h_ref in enumerate(h_refs):
        h_ref[...] = h[i * piece:(i + 1) * piece]


def up(pair, step, z, w):
    d_model, hid = w.shape
    return pl.pallas_call(
        up_kernel,
        grid=(pl.cdiv(hid, UP_TILE),),
        in_specs=[pl.BlockSpec((2 * step, d_model), lambda n: (pair, 0))]
        + [pl.BlockSpec((d_model // UP_SPLIT, UP_TILE), lambda n, s=s: (s, n)) for s in range(UP_SPLIT)],
        out_specs=[pl.BlockSpec((step, UP_TILE), lambda n: (0, n))] * 2,
        out_shape=[jax.ShapeDtypeStruct((step, hid), jnp.bfloat16)] * 2,
        compiler_params=pltpu.CompilerParams(vmem_limit_bytes=VMEM_LIMIT),
        cost_estimate=pl.CostEstimate(flops=4 * step * d_model * hid, bytes_accessed=2 * d_model * hid, transcendentals=2 * step * hid),
    )(z, *[w] * UP_SPLIT)


def down_kernel(meta, *refs):
    n_w = 4 * DOWN_SPLIT
    x_ref, y_ref = refs[-2], refs[-1]
    pieces = y_ref.shape[0] // refs[0].shape[0]
    hs, ws = refs[:4 * pieces], refs[4 * pieces:-2]
    depth = ws[0].shape[0]

    def product(ws):
        branch = None
        for j in range(4):
            for s in range(DOWN_SPLIT):
                parts = [h[:, s * depth:(s + 1) * depth] for h in hs[j * pieces:(j + 1) * pieces]]
                lhs = parts[0] if pieces == 1 else jnp.concatenate(parts, axis=0)
                term = jnp.dot(lhs, ws[j * DOWN_SPLIT + s][...], preferred_element_type=jnp.float32)
                branch = term if branch is None else branch + term
        y_ref[...] = (x_ref[...].astype(jnp.float32) + branch).astype(jnp.bfloat16)

    if len(ws) == n_w:
        product(ws)
    else:
        first = pl.program_id(0) < FIRST_COLS // DOWN_TILE
        pl.when(first)(lambda: product(ws[:n_w]))
        pl.when(jnp.logical_not(first))(lambda: product(ws[n_w:]))


def down(meta, at, step, hs, ws, x, x_col):
    pieces = len(hs[0])
    hid = hs[0][0].shape[1]
    rows = step * pieces
    cols = sum(w.shape[1] for w in ws)
    w_specs, operands, start = [], [], 0
    for w in ws:
        tiles = w.shape[1] // DOWN_TILE
        for j in range(4):
            for s in range(DOWN_SPLIT):
                def index(n, m, j=j, s=s, start=start, tiles=tiles):
                    return (m[j] * DOWN_SPLIT + s, jnp.clip(n - start, 0, tiles - 1))

                w_specs.append(pl.BlockSpec((hid // DOWN_SPLIT, DOWN_TILE), index))
                operands.append(w)
        start += tiles
    return pl.pallas_call(
        down_kernel,
        grid_spec=pltpu.PrefetchScalarGridSpec(
            num_scalar_prefetch=1,
            grid=(cols // DOWN_TILE,),
            in_specs=[pl.BlockSpec((step, hid), lambda n, m: (0, 0))] * (4 * pieces)
            + w_specs
            + [pl.BlockSpec((rows, DOWN_TILE), lambda n, m: (at, x_col // DOWN_TILE + n))],
            out_specs=pl.BlockSpec((rows, DOWN_TILE), lambda n, m: (0, n)),
        ),
        out_shape=jax.ShapeDtypeStruct((rows, cols), jnp.bfloat16),
        compiler_params=pltpu.CompilerParams(vmem_limit_bytes=VMEM_LIMIT),
        cost_estimate=pl.CostEstimate(flops=8 * rows * hid * cols, bytes_accessed=8 * hid * cols, transcendentals=0),
    )(meta, *[h for owner in hs for h in owner], *operands, x)


def copy_kernel(in_ref, out_ref):
    out_ref[...] = in_ref[...]


def solution(mesh):
    n_col = mesh.shape["col"]
    tok_spec = P(("dp", "row"), "col")
    near_pairs = [(i, i ^ 1) for i in range(n_col)]
    far_pairs = [(i, n_col - 1 - i) for i in range(n_col)]

    def near(v):
        return lax.ppermute(v, "col", near_pairs)

    def far(v):
        return lax.ppermute(v, "col", far_pairs)

    def gather(v):
        return lax.all_gather(v, "row", axis=0, tiled=True)

    def local_block(x_loc, gamma_loc, w_in_loc, w_out_loc):
        rows, width = x_loc.shape
        half = rows // 2
        step = half // CHUNKS
        me = lax.axis_index("col")
        side = me // 2
        meta = jnp.stack([me, me ^ 1, n_col - 1 - me, me ^ 2]).astype(jnp.int32)

        w_in_panel = gather(w_in_loc)

        x_mine = lax.dynamic_slice(x_loc, (side * half, 0), (half, width))
        x_other = lax.dynamic_slice(x_loc, ((1 - side) * half, 0), (half, width))
        gamma_row = gamma_loc.reshape(1, width)
        g_near, g_far = near(gamma_row), far(gamma_row)
        g_opp = near(g_far)
        gammas = [gamma_row, g_near, g_far, g_opp]
        a1 = near(x_mine)
        b1 = far(x_other)
        w_out_far = far(w_out_loc)
        b2 = far(x_mine)
        a2 = near(b1)
        a3 = near(x_other)
        b3 = far(a1)

        marked = pl.pallas_call(copy_kernel, out_shape=jax.ShapeDtypeStruct(gamma_row.shape, gamma_row.dtype))(gamma_row)
        w_first, w_last = w_out_loc[:, :FIRST_COLS], w_out_loc[:, FIRST_COLS:]
        w_out_far, marked, w_first, w_last = lax.optimization_barrier((w_out_far, marked, w_first, w_last))
        other_gammas = [marked] + gammas[1:]

        far_panel = gather(w_out_far)
        own_first = gather(w_first)
        own_last = gather(w_last)

        h_mine, h_near, h_other, h_far = [], [], [], []
        z_mine = norm(meta, [x_mine, a1, b1, a2], gammas)
        z_other = norm(meta, [x_other, a3, b2, b3], other_gammas)
        for p in range(CHUNKS // 2):
            h_mine += up(p, step, z_mine, w_in_panel)
            h_near += [near(h_mine[c]) for c in (2 * p, 2 * p + 1)]
        for p in range(CHUNKS // 2):
            h_other += up(p, step, z_other, w_in_panel)
            h_far += [far(h_other[c]) for c in (2 * p, 2 * p + 1)]
        h_opp = [near(h) for h in h_far]

        def call(chunks, ws, x, x_col):
            hs = [[h[c] for c in chunks] for h in (h_mine, h_near, h_far, h_opp)]
            return down(meta, chunks[0] // len(chunks), step, hs, ws, x, x_col)

        y = jnp.zeros((rows, width), jnp.bfloat16)
        for chunks in ((0, 1), (2,), (3,)):
            part = far(call(chunks, [far_panel], b1, 0))
            y = lax.dynamic_update_slice(y, part, ((1 - side) * half + chunks[0] * step, 0))
        part = call((0, 1), [own_first], x_mine, 0)
        y = lax.dynamic_update_slice(y, part, (side * half, 0))
        part = call((0, 1), [own_last], x_mine, FIRST_COLS)
        y = lax.dynamic_update_slice(y, part, (side * half, FIRST_COLS))
        part = call((2, 3), [own_first, own_last], x_mine, 0)
        y = lax.dynamic_update_slice(y, part, (side * half + 2 * step, 0))
        return y

    return jax.shard_map(local_block, mesh=mesh, in_specs=(tok_spec, P("col"), P("row", "col"), P("row", "col")), out_specs=tok_spec, check_vma=False)
```

```python
import functools

import jax
import jax.numpy as jnp
from jax import lax
from jax.experimental import pallas as pl
from jax.experimental.pallas import tpu as pltpu
from jax.sharding import PartitionSpec as P


LN_EPS = 1e-5
CHUNKS = 4
FIRST_COLS = 1024
NORM_ROWS = 128
VMEM_LIMIT = 58 * 1024 * 1024
UP_SPLIT, UP_TILE = 4, 512
DOWN_SPLIT, DOWN_TILE = 2, 256


def norm_kernel(meta, *refs):
    blocks, gammas, z_ref = refs[0:4], refs[4:8], refs[8]
    width = blocks[0].shape[1]
    d_model = z_ref.shape[1]
    sums, squares = 0.0, 0.0
    for b in blocks:
        v = b[...].astype(jnp.float32)
        sums += jnp.sum(v, axis=1, keepdims=True)
        squares += jnp.sum(v * v, axis=1, keepdims=True)
    mean = sums / d_model
    scale = lax.rsqrt(squares / d_model - mean * mean + LN_EPS)
    for j, (b, g) in enumerate(zip(blocks, gammas)):
        piece = (b[...].astype(jnp.float32) - mean) * scale * g[...]
        z_ref[:, pl.ds(pl.multiple_of(meta[j] * width, 128), width)] = piece.astype(jnp.bfloat16)


def norm(meta, blocks, gammas):
    rows, width = blocks[0].shape
    d_model = width * 4
    return pl.pallas_call(
        norm_kernel,
        grid_spec=pltpu.PrefetchScalarGridSpec(
            num_scalar_prefetch=1,
            grid=(rows // NORM_ROWS,),
            in_specs=[pl.BlockSpec((NORM_ROWS, width), lambda i, m: (i, 0))] * 4
            + [pl.BlockSpec((1, width), lambda i, m: (0, 0))] * 4,
            out_specs=pl.BlockSpec((NORM_ROWS, d_model), lambda i, m: (i, 0)),
        ),
        out_shape=jax.ShapeDtypeStruct((rows, d_model), jnp.bfloat16),
        compiler_params=pltpu.CompilerParams(vmem_limit_bytes=VMEM_LIMIT),
        cost_estimate=pl.CostEstimate(flops=64 * rows * d_model, bytes_accessed=4 * rows * d_model, transcendentals=rows),
    )(meta, *blocks, *gammas)


def up_kernel(z_ref, *refs):
    ws, h_refs = refs[:UP_SPLIT], refs[UP_SPLIT:]
    depth = ws[0].shape[0]
    pre = jnp.dot(z_ref[:, :depth], ws[0][...], preferred_element_type=jnp.float32)
    for s in range(1, UP_SPLIT):
        pre += jnp.dot(z_ref[:, s * depth:(s + 1) * depth], ws[s][...], preferred_element_type=jnp.float32)
    h = jax.nn.gelu(pre, approximate=True).astype(jnp.bfloat16)
    piece = h_refs[0].shape[0]
    for i, h_ref in enumerate(h_refs):
        h_ref[...] = h[i * piece:(i + 1) * piece]


def up(pair, step, z, w):
    d_model, hid = w.shape
    return pl.pallas_call(
        up_kernel,
        grid=(pl.cdiv(hid, UP_TILE),),
        in_specs=[pl.BlockSpec((2 * step, d_model), lambda n: (pair, 0))]
        + [pl.BlockSpec((d_model // UP_SPLIT, UP_TILE), lambda n, s=s: (s, n)) for s in range(UP_SPLIT)],
        out_specs=[pl.BlockSpec((step, UP_TILE), lambda n: (0, n))] * 2,
        out_shape=[jax.ShapeDtypeStruct((step, hid), jnp.bfloat16)] * 2,
        compiler_params=pltpu.CompilerParams(vmem_limit_bytes=VMEM_LIMIT),
        cost_estimate=pl.CostEstimate(flops=4 * step * d_model * hid, bytes_accessed=2 * d_model * hid, transcendentals=2 * step * hid),
    )(z, *[w] * UP_SPLIT)


def down_kernel(n_owner, pieces, final, with_part, meta, *refs):
    refs = list(refs)
    y_ref = refs.pop()
    x_ref = refs.pop() if final else None
    part_ref = refs.pop() if with_part else None
    hs, ws = refs[:n_owner * pieces], refs[n_owner * pieces:]
    depth = ws[0].shape[0]
    branch = part_ref[...] if with_part else None
    for j in range(n_owner):
        for s in range(DOWN_SPLIT):
            parts = [h[:, s * depth:(s + 1) * depth] for h in hs[j * pieces:(j + 1) * pieces]]
            lhs = parts[0] if pieces == 1 else jnp.concatenate(parts, axis=0)
            term = jnp.dot(lhs, ws[j * DOWN_SPLIT + s][...], preferred_element_type=jnp.float32)
            branch = term if branch is None else branch + term
    if final:
        branch = x_ref[...].astype(jnp.float32) + branch
    y_ref[...] = branch.astype(y_ref.dtype)


def down(meta, at, step, hs, owners, w, part=None, x=None, x_col=0):
    pieces = len(hs[0])
    hid = hs[0][0].shape[1]
    rows = step * pieces
    cols = w.shape[1]
    n_owner = len(owners)
    once = pl.Buffered(buffer_count=1)
    specs = [pl.BlockSpec((step, hid), lambda n, m: (0, 0), pipeline_mode=once)] * (n_owner * pieces)
    specs += [
        pl.BlockSpec((hid // DOWN_SPLIT, DOWN_TILE), lambda n, m, j=j, s=s: (m[j] * DOWN_SPLIT + s, n))
        for j in owners for s in range(DOWN_SPLIT)
    ]
    operands = [h for owner in hs for h in owner] + [w] * (n_owner * DOWN_SPLIT)
    if part is not None:
        specs.append(pl.BlockSpec((rows, DOWN_TILE), lambda n, m: (at, n)))
        operands.append(part)
    if x is not None:
        specs.append(pl.BlockSpec((rows, DOWN_TILE), lambda n, m: (at, x_col // DOWN_TILE + n)))
        operands.append(x)
    return pl.pallas_call(
        functools.partial(down_kernel, n_owner, pieces, x is not None, part is not None),
        grid_spec=pltpu.PrefetchScalarGridSpec(
            num_scalar_prefetch=1,
            grid=(cols // DOWN_TILE,),
            in_specs=specs,
            out_specs=pl.BlockSpec((rows, DOWN_TILE), lambda n, m: (0, n)),
        ),
        out_shape=jax.ShapeDtypeStruct((rows, cols), jnp.float32 if x is None else jnp.bfloat16),
        compiler_params=pltpu.CompilerParams(vmem_limit_bytes=VMEM_LIMIT),
        cost_estimate=pl.CostEstimate(flops=2 * n_owner * rows * hid * cols, bytes_accessed=2 * n_owner * hid * cols, transcendentals=0),
    )(meta, *operands)


def copy_kernel(in_ref, out_ref):
    out_ref[...] = in_ref[...]


def solution(mesh):
    n_col = mesh.shape["col"]
    tok_spec = P(("dp", "row"), "col")
    near_pairs = [(i, i ^ 1) for i in range(n_col)]
    far_pairs = [(i, n_col - 1 - i) for i in range(n_col)]

    def near(v):
        return lax.ppermute(v, "col", near_pairs)

    def far(v):
        return lax.ppermute(v, "col", far_pairs)

    def gather(v):
        return lax.all_gather(v, "row", axis=0, tiled=True)

    def local_block(x_loc, gamma_loc, w_in_loc, w_out_loc):
        rows, width = x_loc.shape
        half = rows // 2
        step = half // CHUNKS
        me = lax.axis_index("col")
        side = me // 2
        meta = jnp.stack([me, me ^ 1, n_col - 1 - me, me ^ 2]).astype(jnp.int32)

        w_in_panel = gather(w_in_loc)

        x_mine = lax.dynamic_slice(x_loc, (side * half, 0), (half, width))
        x_other = lax.dynamic_slice(x_loc, ((1 - side) * half, 0), (half, width))
        gamma_row = gamma_loc.reshape(1, width)
        g_near, g_far = near(gamma_row), far(gamma_row)
        g_opp = near(g_far)
        gammas = [gamma_row, g_near, g_far, g_opp]
        a1 = near(x_mine)
        b1 = far(x_other)
        w_out_far = far(w_out_loc)
        b2 = far(x_mine)
        a2 = near(b1)
        a3 = near(x_other)
        b3 = far(a1)

        marked = pl.pallas_call(copy_kernel, out_shape=jax.ShapeDtypeStruct(gamma_row.shape, gamma_row.dtype))(gamma_row)
        w_first, w_last = w_out_loc[:, :FIRST_COLS], w_out_loc[:, FIRST_COLS:]
        w_out_far, marked, w_first, w_last = lax.optimization_barrier((w_out_far, marked, w_first, w_last))
        other_gammas = [marked] + gammas[1:]

        far_panel = gather(w_out_far)
        own_first = gather(w_first)
        own_last = gather(w_last)

        h_mine, h_near, h_other, h_far = [], [], [], []
        z_mine = norm(meta, [x_mine, a1, b1, a2], gammas)
        z_other = norm(meta, [x_other, a3, b2, b3], other_gammas)
        for p in range(CHUNKS // 2):
            h_mine += up(p, step, z_mine, w_in_panel)
            h_near += [near(h_mine[c]) for c in (2 * p, 2 * p + 1)]
        for p in range(CHUNKS // 2):
            h_other += up(p, step, z_other, w_in_panel)
            h_far += [far(h_other[c]) for c in (2 * p, 2 * p + 1)]
        h_opp = [near(h) for h in h_far]

        pieces = (h_mine, h_near, h_far, h_opp)

        def call(chunks, owners, w, **rest):
            return down(meta, chunks[0] // len(chunks), step, [[pieces[j][c] for c in chunks] for j in owners], owners, w, **rest)

        every = tuple(range(CHUNKS))
        y = jnp.zeros((rows, width), jnp.bfloat16)
        far_part = call(every, (0, 1), far_panel)
        for chunks in ((0, 1), (2,), (3,)):
            done = call(chunks, (2, 3), far_panel, part=far_part, x=b1)
            y = lax.dynamic_update_slice(y, far(done), ((1 - side) * half + chunks[0] * step, 0))
        own_part = call(every, (0, 1, 2), own_first)
        done = call(every, (3,), own_first, part=own_part, x=x_mine)
        y = lax.dynamic_update_slice(y, done, (side * half, 0))
        done = call(every, (0, 1, 2, 3), own_last, x=x_mine, x_col=FIRST_COLS)
        y = lax.dynamic_update_slice(y, done, (side * half, FIRST_COLS))
        return y

    return jax.shard_map(local_block, mesh=mesh, in_specs=(tok_spec, P("col"), P("row", "col"), P("row", "col")), out_specs=tok_spec, check_vma=False)
```

```python
import functools

import jax
import jax.numpy as jnp
from jax import lax
from jax.experimental import pallas as pl
from jax.experimental.pallas import tpu as pltpu
from jax.sharding import PartitionSpec as P


LN_EPS = 1e-5
CHUNKS = 4
FIRST_COLS = 768
NORM_ROWS = 128
VMEM_LIMIT = 58 * 1024 * 1024
UP_SPLIT, UP_TILE = 4, 512
DOWN_SPLIT, DOWN_TILE = 2, 256


def norm_kernel(meta, *refs):
    blocks, gammas, z_ref = refs[0:4], refs[4:8], refs[8]
    width = blocks[0].shape[1]
    d_model = z_ref.shape[1]
    sums, squares = 0.0, 0.0
    for b in blocks:
        v = b[...].astype(jnp.float32)
        sums += jnp.sum(v, axis=1, keepdims=True)
        squares += jnp.sum(v * v, axis=1, keepdims=True)
    mean = sums / d_model
    scale = lax.rsqrt(squares / d_model - mean * mean + LN_EPS)
    for j, (b, g) in enumerate(zip(blocks, gammas)):
        piece = (b[...].astype(jnp.float32) - mean) * scale * g[...]
        z_ref[:, pl.ds(pl.multiple_of(meta[j] * width, 128), width)] = piece.astype(jnp.bfloat16)


def norm(meta, at, rows, blocks, gammas):
    width = blocks[0].shape[1]
    d_model = width * 4
    return pl.pallas_call(
        norm_kernel,
        grid_spec=pltpu.PrefetchScalarGridSpec(
            num_scalar_prefetch=1,
            grid=(rows // NORM_ROWS,),
            in_specs=[pl.BlockSpec((NORM_ROWS, width), lambda i, m: (at * (rows // NORM_ROWS) + i, 0))] * 4
            + [pl.BlockSpec((1, width), lambda i, m: (0, 0))] * 4,
            out_specs=pl.BlockSpec((NORM_ROWS, d_model), lambda i, m: (i, 0)),
        ),
        out_shape=jax.ShapeDtypeStruct((rows, d_model), jnp.bfloat16),
        compiler_params=pltpu.CompilerParams(vmem_limit_bytes=VMEM_LIMIT),
        cost_estimate=pl.CostEstimate(flops=64 * rows * d_model, bytes_accessed=4 * rows * d_model, transcendentals=rows),
    )(meta, *blocks, *gammas)


def up_kernel(z_ref, *refs):
    ws, h_refs = refs[:UP_SPLIT], refs[UP_SPLIT:]
    depth = ws[0].shape[0]
    pre = jnp.dot(z_ref[:, :depth], ws[0][...], preferred_element_type=jnp.float32)
    for s in range(1, UP_SPLIT):
        pre += jnp.dot(z_ref[:, s * depth:(s + 1) * depth], ws[s][...], preferred_element_type=jnp.float32)
    h = jax.nn.gelu(pre, approximate=True).astype(jnp.bfloat16)
    piece = h_refs[0].shape[0]
    for i, h_ref in enumerate(h_refs):
        h_ref[...] = h[i * piece:(i + 1) * piece]


def up(pair, step, z, w):
    d_model, hid = w.shape
    return pl.pallas_call(
        up_kernel,
        grid=(pl.cdiv(hid, UP_TILE),),
        in_specs=[pl.BlockSpec((2 * step, d_model), lambda n: (pair, 0))]
        + [pl.BlockSpec((d_model // UP_SPLIT, UP_TILE), lambda n, s=s: (s, n)) for s in range(UP_SPLIT)],
        out_specs=[pl.BlockSpec((step, UP_TILE), lambda n: (0, n))] * 2,
        out_shape=[jax.ShapeDtypeStruct((step, hid), jnp.bfloat16)] * 2,
        compiler_params=pltpu.CompilerParams(vmem_limit_bytes=VMEM_LIMIT),
        cost_estimate=pl.CostEstimate(flops=4 * step * d_model * hid, bytes_accessed=2 * d_model * hid, transcendentals=2 * step * hid),
    )(z, *[w] * UP_SPLIT)


def down_kernel(n_owner, pieces, final, with_part, meta, *refs):
    refs = list(refs)
    y_ref = refs.pop()
    x_ref = refs.pop() if final else None
    part_ref = refs.pop() if with_part else None
    hs, ws = refs[:n_owner * pieces], refs[n_owner * pieces:]
    depth = ws[0].shape[0]
    branch = part_ref[...] if with_part else None
    for j in range(n_owner):
        for s in range(DOWN_SPLIT):
            parts = [h[:, s * depth:(s + 1) * depth] for h in hs[j * pieces:(j + 1) * pieces]]
            lhs = parts[0] if pieces == 1 else jnp.concatenate(parts, axis=0)
            term = jnp.dot(lhs, ws[j * DOWN_SPLIT + s][...], preferred_element_type=jnp.float32)
            branch = term if branch is None else branch + term
    if final:
        branch = x_ref[...].astype(jnp.float32) + branch
    y_ref[...] = branch.astype(y_ref.dtype)


def down(meta, at, step, hs, owners, w, part=None, part_at=0, x=None, x_col=0):
    pieces = len(hs[0])
    hid = hs[0][0].shape[1]
    rows = step * pieces
    cols = w.shape[1]
    n_owner = len(owners)
    once = pl.Buffered(buffer_count=1)
    specs = [pl.BlockSpec((step, hid), lambda n, m: (0, 0), pipeline_mode=once)] * (n_owner * pieces)
    specs += [
        pl.BlockSpec((hid // DOWN_SPLIT, DOWN_TILE), lambda n, m, j=j, s=s: (m[j] * DOWN_SPLIT + s, n))
        for j in owners for s in range(DOWN_SPLIT)
    ]
    operands = [h for owner in hs for h in owner] + [w] * (n_owner * DOWN_SPLIT)
    if part is not None:
        specs.append(pl.BlockSpec((rows, DOWN_TILE), lambda n, m: (part_at, n)))
        operands.append(part)
    if x is not None:
        specs.append(pl.BlockSpec((rows, DOWN_TILE), lambda n, m: (at, x_col // DOWN_TILE + n)))
        operands.append(x)
    return pl.pallas_call(
        functools.partial(down_kernel, n_owner, pieces, x is not None, part is not None),
        grid_spec=pltpu.PrefetchScalarGridSpec(
            num_scalar_prefetch=1,
            grid=(cols // DOWN_TILE,),
            in_specs=specs,
            out_specs=pl.BlockSpec((rows, DOWN_TILE), lambda n, m: (0, n)),
        ),
        out_shape=jax.ShapeDtypeStruct((rows, cols), jnp.float32 if x is None else jnp.bfloat16),
        compiler_params=pltpu.CompilerParams(vmem_limit_bytes=VMEM_LIMIT),
        cost_estimate=pl.CostEstimate(flops=2 * n_owner * rows * hid * cols, bytes_accessed=2 * n_owner * hid * cols, transcendentals=0),
    )(meta, *operands)


def copy_kernel(in_ref, out_ref):
    out_ref[...] = in_ref[...]


def solution(mesh):
    n_col = mesh.shape["col"]
    tok_spec = P(("dp", "row"), "col")
    near_pairs = [(i, i ^ 1) for i in range(n_col)]
    far_pairs = [(i, n_col - 1 - i) for i in range(n_col)]

    def near(v):
        return lax.ppermute(v, "col", near_pairs)

    def far(v):
        return lax.ppermute(v, "col", far_pairs)

    def gather(v):
        return lax.all_gather(v, "row", axis=0, tiled=True)

    def local_block(x_loc, gamma_loc, w_in_loc, w_out_loc):
        rows, width = x_loc.shape
        half = rows // 2
        step = half // CHUNKS
        me = lax.axis_index("col")
        side = me // 2
        meta = jnp.stack([me, me ^ 1, n_col - 1 - me, me ^ 2]).astype(jnp.int32)

        w_in_panel = gather(w_in_loc)

        x_mine = lax.dynamic_slice(x_loc, (side * half, 0), (half, width))
        x_other = lax.dynamic_slice(x_loc, ((1 - side) * half, 0), (half, width))
        gamma_row = gamma_loc.reshape(1, width)
        g_near, g_far = near(gamma_row), far(gamma_row)
        g_opp = near(g_far)
        gammas = [gamma_row, g_near, g_far, g_opp]
        a1 = near(x_mine)
        b1 = far(x_other)
        w_out_far = far(w_out_loc)
        b2 = far(x_mine)
        a2 = near(b1)
        a3 = near(x_other)
        b3 = far(a1)

        marked = pl.pallas_call(copy_kernel, out_shape=jax.ShapeDtypeStruct(gamma_row.shape, gamma_row.dtype))(gamma_row)
        w_first, w_last = w_out_loc[:, :FIRST_COLS], w_out_loc[:, FIRST_COLS:]
        w_out_far, marked, w_first, w_last = lax.optimization_barrier((w_out_far, marked, w_first, w_last))
        other_gammas = [marked] + gammas[1:]

        far_panel = gather(w_out_far)
        own_first = gather(w_first)
        own_last = gather(w_last)

        h_mine, h_near, h_other, h_far = [], [], [], []
        z_mine = norm(meta, 0, half, [x_mine, a1, b1, a2], gammas)
        for p in range(CHUNKS // 2):
            h_mine += up(p, step, z_mine, w_in_panel)
            h_near += [near(h_mine[c]) for c in (2 * p, 2 * p + 1)]
        for p in range(CHUNKS // 2):
            z_other = norm(meta, p, 2 * step, [x_other, a3, b2, b3], other_gammas)
            h_other += up(0, step, z_other, w_in_panel)
            h_far += [far(h_other[c]) for c in (2 * p, 2 * p + 1)]
        h_opp = [near(h) for h in h_far]

        pieces = (h_mine, h_near, h_far, h_opp)

        def call(chunks, owners, w, **rest):
            return down(meta, chunks[0] // len(chunks), step, [[pieces[j][c] for c in chunks] for j in owners], owners, w, **rest)

        every = tuple(range(CHUNKS))
        y = jnp.zeros((rows, width), jnp.bfloat16)
        far_part = call(every, (0, 1), far_panel)
        for chunks in ((0, 1), (2,), (3,)):
            done = call(chunks, (2, 3), far_panel, part=far_part, part_at=chunks[0] // len(chunks), x=b1)
            y = lax.dynamic_update_slice(y, far(done), ((1 - side) * half + chunks[0] * step, 0))
        for pair in ((0, 1), (2, 3)):
            own_part = call(pair, (0, 1, 2), own_first)
            done = call(pair, (3,), own_first, part=own_part, x=x_mine)
            y = lax.dynamic_update_slice(y, done, (side * half + pair[0] * step, 0))
        done = call(every, (0, 1, 2, 3), own_last, x=x_mine, x_col=FIRST_COLS)
        y = lax.dynamic_update_slice(y, done, (side * half, FIRST_COLS))
        return y

    return jax.shard_map(local_block, mesh=mesh, in_specs=(tok_spec, P("col"), P("row", "col"), P("row", "col")), out_specs=tok_spec, check_vma=False)
```
